32 devices in a mesh: cfg: 2 (over y), space: 4 (over z), tm: 4 (over x, core).
Axes of the slice: x: 2, y: 2, z: 4, core: 2. Of those that a mesh axis runs over, the one named last changes fastest.
Arguments:
- solutions: bfloat16 [16, 128, 32, 3072], P(('cfg', 'tm'), None, None, 'space'), parts along dimension 0, may hold values from -6 to 6
- eigvecs: bfloat16 [16, 2, 128, 3072], P(('cfg', 'tm'), None, 'space'), parts along dimension 0, may hold values from -0.078125 to 0.078125
- source_time: int32 [256], P('cfg'), parts along dimension 0, may hold values from 0 to 7
Outputs:
- perambulator: bfloat16 [16, 128, 32, 128], P(('cfg', 'tm'), 'space'), parts along dimension 0
The draws below stay inside these ranges and needn't reach their ends.
There are 2 independent parts, one for each index of `cfg`. The reference program is written for one: setup_inputs(seed, part) draws one part's arguments, and reference() takes and returns one part's arrays. A program takes and returns all parts, laid end to end along the dimension named above; each array names one. Nothing has to cross between parts.
All inputs are finite; a program needn't handle non-finite values.
Results may differ from the reference program's by a relative error of at most 0.001.
Values may be sent and summed in bfloat16 or wider, within the bound.
A program may use at most 128 MiB of HBM per device.

```python
import jax
import jax.numpy as jnp
from jax import lax

NVEC = 128
NSRC = 128
NT = 8
CV = 3072


def place_ends(array, key, low, high):
    extent = array.shape
    spot = [jax.random.randint(jax.random.fold_in(key, axis), (), 0, extent[axis]) for axis in range(len(extent))]
    array = array.at[tuple(spot)].set(low)
    longest = extent.index(max(extent))
    spot[longest] = (spot[longest] + 1) % extent[longest]
    return array.at[tuple(spot)].set(high)


def strengthened(values, key, source, target, blocks, factor):
    owner, partner = [(jnp.arange(values.shape[position]) // (values.shape[position] // blocks)).reshape([-1 if axis == position else 1 for axis in range(values.ndim)]) for position in (source, target)]
    chosen = jax.random.permutation(key, blocks)[partner]
    strong = (owner == chosen) | (owner == (partner + blocks // 2) % blocks)
    return jnp.where(strong, factor * values, values)


def shard_levels(key, dims, cuts, low, high):
    def one(dim, parts):
        steps = jax.random.uniform(jax.random.fold_in(jax.random.fold_in(key, 6), dim), (parts,), jnp.float32, low / len(cuts), high / len(cuts))
        return jnp.repeat(jnp.exp(steps), dims[dim] // parts).reshape((-1,) + (1,) * (len(dims) - dim - 1))

    factor_of = one(*cuts[0])
    for cut in cuts[1:]:
        factor_of = factor_of * one(*cut)
    return factor_of


def gaussian(own_key, extent, width, limit, cuts=(), kind=jnp.bfloat16):
    drawn = width * jax.random.normal(own_key, extent, jnp.float32)
    if cuts:
        drawn = drawn * shard_levels(own_key, extent, cuts, -0.22, 0.18)
    return jnp.clip(drawn, -limit, limit).astype(kind)


def heavy_noise(rng, dims, spread, bound, cuts, heavy, kind=jnp.bfloat16):
    drawn = spread * jax.random.normal(rng, dims, jnp.float32)
    if cuts:
        drawn = drawn * shard_levels(rng, dims, cuts, -0.22, 0.18)
    return jnp.clip(strengthened(drawn, jax.random.fold_in(rng, 3), *heavy), -bound, bound).astype(kind)


def setup_inputs(seed: int = 0, part: int = 0) -> dict:
    key_of = jax.random.split(jax.random.key(seed), 4)
    part_splits = jax.random.split(jax.random.fold_in(key_of[3], part), 4)
    solutions = heavy_noise(part_splits[0], (NT, NSRC, 32, CV), 1.0, 6.0, ((0, 4), (3, 4)), (3, 1, 4, 2.0))
    eigvecs = gaussian(part_splits[1], (NT, 2, NVEC, CV), (2 * CV) ** -0.5, 0.078125, ((0, 4), (2, 4)))
    source_time = place_ends(jax.random.randint(part_splits[2], (NSRC,), 0, NT), jax.random.fold_in(part_splits[2], 1), 0, NT - 1).astype(jnp.int32)
    return {"solutions": solutions, "eigvecs": eigvecs, "source_time": source_time}


def contract_slice(spinors, vectors):
    sources = spinors.shape[0]
    count = vectors.shape[1]
    stacked = vectors.reshape(2 * count, vectors.shape[2])
    products = jnp.dot(spinors.reshape(sources * 32, spinors.shape[2]), stacked.T, precision=lax.Precision.HIGHEST, preferred_element_type=jnp.float32)
    products = products.reshape(sources, 2, 16, 2, count)
    real_part = products[:, 0, :, 0, :] + products[:, 1, :, 1, :]
    imag_part = products[:, 1, :, 0, :] - products[:, 0, :, 1, :]
    return jnp.concatenate([real_part, imag_part], axis=1)


def reference(solutions, eigvecs, source_time):
    def one_slice(pair):
        return contract_slice(pair[0].astype(jnp.float32), pair[1].astype(jnp.float32))

    sums = lax.map(one_slice, (solutions, eigvecs))
    times = jnp.arange(NT, dtype=jnp.int32)
    signs = jnp.where(times[:, None] < source_time[None, :], -1.0, 1.0).astype(jnp.float32)
    return (sums * signs[:, :, None, None]).astype(jnp.bfloat16)
```

```python
import functools

import jax
import jax.numpy as jnp
from jax import lax
from jax.experimental import pallas as pl
from jax.experimental.pallas import tpu as pltpu
from jax.sharding import PartitionSpec as P

MESH = pl.DeviceIdType.MESH
LEVELS = 32767.0


def kernel(n, time_ref, sol_ref, eig_ref, out_ref, sol_v, eig_v, w_v, part, own, code, scale, code_in, scale_in,
           sol_sem, own_sem, eig_send, eig_recv, code_send, scale_send, code_recv, scale_recv):
    me = lax.axis_index("space")
    slices, sources, spins, cols = sol_v.shape
    count = eig_ref.shape[2]
    vectors = n * count
    owned = sources // n
    half = spins // 2

    barrier = pltpu.get_barrier_semaphore()
    for o in range(1, n):
        pl.semaphore_signal(barrier, inc=1, device_id={"space": lax.rem(me + o, n)}, device_id_type=MESH)

    def block_of(d):
        return pl.ds(pl.multiple_of(d * cols, cols), cols)

    def eig_own(t):
        return pltpu.make_async_copy(eig_ref.at[t, :, :, block_of(me)], eig_v.at[t, me], own_sem.at[t])

    def sol_copy(t, d):
        rows = pl.ds(d * owned, owned)
        return pltpu.make_async_copy(sol_ref.at[t, rows], sol_v.at[t, rows], sol_sem.at[t, d])

    def eig_copy(t, o, dst):
        to = lax.rem(me + o, n)
        return pltpu.make_async_remote_copy(
            eig_ref.at[t, :, :, block_of(to)], eig_v.at[t, dst], eig_send.at[t, o], eig_recv.at[t, o],
            device_id={"space": to}, device_id_type=MESH)

    for t in range(slices):
        eig_own(t).start()

    def start_sol(t):
        def body(d, _):
            sol_copy(t, d).start()
            return 0
        lax.fori_loop(0, n, body, 0)

    start_sol(0)
    pl.semaphore_wait(barrier, n - 1)
    for o in range(1, n):
        eig_copy(0, o, me).start()
    for t in range(1, slices):
        start_sol(t)

    def partial_sum(t, d, dst):
        block = sol_v[t, pl.ds(d * owned, owned)].reshape(owned * spins, cols)
        p = lax.dot_general(block, w_v[t], (((1,), (1,)), ((), ())), preferred_element_type=jnp.float32)
        p = p.reshape(owned, 2, half, 2 * vectors)
        dst[:, :half, :] = p[:, 0, :, :vectors] + p[:, 1, :, vectors:]
        dst[:, half:, :] = p[:, 1, :, :vectors] - p[:, 0, :, vectors:]

    def chunk_copies(way, t, d):
        to = lax.rem(jnp.where(way == 0, me + 1, me + n - 1), n)
        return [
            pltpu.make_async_remote_copy(src.at[t, d], dst.at[way, t, d], s.at[t, d], r.at[way, t, d],
                                         device_id={"space": to}, device_id_type=MESH)
            for src, dst, s, r in ((code, code_in, code_send, code_recv), (scale, scale_in, scale_send, scale_recv))
        ]

    def received(way, t, d):
        for c in chunk_copies(way, t, d):
            c.wait_recv()
        return code_in[way, t, d].astype(jnp.int32).astype(jnp.float32) * scale_in[way, t, d][:1][None]

    def emit(t):
        def body(j, _):
            k = j // 2
            way = jnp.where(me < n // 2, j % 2, 1 - j % 2)
            d = jnp.where(way == 0, n - 1 - k, k)

            @pl.when(jnp.where(way == 0, d - me, me - d) > 0)
            def _():
                partial_sum(t, d, part)

                @pl.when(jnp.where(way == 0, me, n - 1 - me) > 0)
                def _():
                    part[...] += received(way, t, d)

                x = part[...]
                top = jnp.maximum(jnp.max(jnp.max(jnp.abs(x), axis=0), axis=0, keepdims=True), 1e-33)
                code[t, d] = jnp.round(x * (LEVELS / top)[None]).astype(jnp.int32).astype(jnp.int16)
                scale[t, d] = jnp.broadcast_to(top * (1.0 / LEVELS), (8, vectors))
                for c in chunk_copies(way, t, d):
                    c.start()
            return 0

        lax.fori_loop(0, 2 * (n - 1), body, 0)

    for t in range(slices):
        for o in range(1, n):
            eig_copy(t, o, me).wait_send()
        if t + 1 < slices:
            for o in range(1, n):
                eig_copy(t + 1, o, me).start()
        for o in range(1, n):
            eig_copy(t, o, lax.rem(me + n - o, n)).wait_recv()
        eig_own(t).wait()
        for c in range(2):
            w_v[t, c * vectors:(c + 1) * vectors, :] = (
                eig_v[t, :, c].astype(jnp.float32).reshape(vectors, cols).astype(jnp.bfloat16))

        def wait_sol(d, _):
            sol_copy(t, d).wait()
            return 0

        lax.fori_loop(0, n, wait_sol, 0)
        emit(t)
        partial_sum(t, me, own.at[t])

    for t in range(slices):
        @pl.when(me > 0)
        def _():
            own[t] += received(0, t, me)

        @pl.when(me < n - 1)
        def _():
            own[t] += received(1, t, me)

        now = lax.axis_index("tm") * slices + t

        def finish(i, _):
            sign = jnp.where(now < time_ref[me * owned + i], -1.0, 1.0)
            out_ref[t, i] = (own[t, i] * sign).astype(jnp.bfloat16)
            return 0

        lax.fori_loop(0, owned, finish, 0)

    def drain(j, _):
        t, d = j // n, j % n

        @pl.when(d != me)
        def _():
            for c in chunk_copies(jnp.where(d > me, 0, 1), t, d):
                c.wait_send()
        return 0

    lax.fori_loop(0, slices * n, drain, 0)


def shards(n, solutions, eigvecs, source_time):
    slices, sources, spins, cols = solutions.shape
    count = eigvecs.shape[2]
    vectors = n * count
    owned = sources // n
    dma = pltpu.SemaphoreType.DMA
    return pl.pallas_call(
        functools.partial(kernel, n),
        out_shape=jax.ShapeDtypeStruct((slices, owned, spins, vectors), jnp.bfloat16),
        in_specs=[
            pl.BlockSpec(memory_space=pltpu.SMEM),
            pl.BlockSpec(memory_space=pl.ANY),
            pl.BlockSpec(memory_space=pl.ANY),
        ],
        out_specs=pl.BlockSpec(memory_space=pltpu.VMEM),
        scratch_shapes=[
            pltpu.VMEM((slices, sources, spins, cols), jnp.bfloat16),
            pltpu.VMEM((slices, n, 2, count, cols), jnp.bfloat16),
            pltpu.VMEM((slices, 2 * vectors, cols), jnp.bfloat16),
            pltpu.VMEM((owned, spins, vectors), jnp.float32),
            pltpu.VMEM((slices, owned, spins, vectors), jnp.float32),
            pltpu.VMEM((slices, n, owned, spins, vectors), jnp.int16),
            pltpu.VMEM((slices, n, 8, vectors), jnp.float32),
            pltpu.VMEM((2, slices, n, owned, spins, vectors), jnp.int16),
            pltpu.VMEM((2, slices, n, 8, vectors), jnp.float32),
            dma((slices, n)),
            dma((slices,)),
            dma((slices, n)),
            dma((slices, n)),
            dma((slices, n)),
            dma((slices, n)),
            dma((2, slices, n)),
            dma((2, slices, n)),
        ],
        compiler_params=pltpu.CompilerParams(
            collective_id=0, has_side_effects=True, vmem_limit_bytes=48 << 20),
    )(source_time, solutions, eigvecs)


def solution(mesh):
    return jax.shard_map(
        functools.partial(shards, mesh.shape["space"]),
        mesh=mesh,
        in_specs=(
            P(("cfg", "tm"), None, None, "space"),
            P(("cfg", "tm"), None, "space", None),
            P("cfg"),
        ),
        out_specs=P(("cfg", "tm"), "space", None, None),
        check_vma=False,
    )
```

```python
import functools

import jax
import jax.numpy as jnp
from jax import lax
from jax.experimental import pallas as pl
from jax.experimental.pallas import tpu as pltpu
from jax.sharding import PartitionSpec as P

MESH = pl.DeviceIdType.MESH
LEVELS = 32767.0
PIECES = 2


def kernel(n, pieces, time_hbm, sol_ref, eig_hbm, out_ref, time_ref, eig_ref, sol_v, eig_v, w_v, part, own, code, scale,
           code_in, scale_in, time_sem, load_sem, sol_sem, own_sem, eig_send, eig_recv, code_send, scale_send, code_recv, scale_recv):
    me = lax.axis_index("space")
    slices, sources, spins, cols = sol_v.shape
    count = eig_ref.shape[2]
    vectors = n * count
    owned = sources // n
    piece = owned // pieces
    half = spins // 2
    outer = jnp.where(me < n // 2, me - 1, me + 1)
    is_end = (me == 0) | (me == n - 1)

    barrier = pltpu.get_barrier_semaphore()
    for o in range(1, n):
        pl.semaphore_signal(barrier, inc=1, device_id={"space": lax.rem(me + o, n)}, device_id_type=MESH)

    def block_of(d):
        return pl.ds(pl.multiple_of(d * cols, cols), cols)

    def eig_own(t):
        return pltpu.make_async_copy(eig_hbm.at[t, :, :, block_of(me)], eig_v.at[t, me], own_sem.at[t])

    def eig_load(t):
        return pltpu.make_async_copy(eig_hbm.at[t], eig_ref.at[t], load_sem.at[t])

    def sol_copy(t, d):
        rows = pl.ds(d * owned, owned)
        return pltpu.make_async_copy(sol_ref.at[t, rows], sol_v.at[t, rows], sol_sem.at[t, d])

    def eig_copy(t, o, dst):
        to = lax.rem(me + o, n)
        return pltpu.make_async_remote_copy(
            eig_ref.at[t, :, :, block_of(to)], eig_v.at[t, dst], eig_send.at[t, o], eig_recv.at[t, o],
            device_id={"space": to}, device_id_type=MESH)

    for t in range(slices):
        eig_load(t).start()
    time_copy = pltpu.make_async_copy(time_hbm, time_ref, time_sem)
    time_copy.start()
    for t in range(slices):
        eig_own(t).start()

    def start_sol(t):
        def body(d, _):
            sol_copy(t, d).start()
            return 0
        lax.fori_loop(0, n, body, 0)

    far_first = sorted(range(1, n), key=lambda o: -min(o, n - o))
    eig_load(0).wait()
    pl.semaphore_wait(barrier, n - 1)
    for o in far_first:
        eig_copy(0, o, me).start()
    for t in range(slices):
        start_sol(t)
    for t in range(1, slices):
        eig_load(t).wait()
    time_copy.wait()

    def partial_sum(t, q, dst):
        block = sol_v[t, pl.ds(q * piece, piece)].reshape(piece * spins, cols)
        p = lax.dot_general(block, w_v[t], (((1,), (1,)), ((), ())), preferred_element_type=jnp.float32)
        p = p.reshape(piece, 2, half, 2 * vectors)
        dst[:, :half, :] = p[:, 0, :, :vectors] + p[:, 1, :, vectors:]
        dst[:, half:, :] = p[:, 1, :, :vectors] - p[:, 0, :, vectors:]

    def chunk_copies(way, t, d):
        to = lax.rem(jnp.where(way == 0, me + 1, me + n - 1), n)
        return [
            pltpu.make_async_remote_copy(src.at[t, d], dst.at[way, t, d], s.at[t, d], r.at[way, t, d],
                                         device_id={"space": to}, device_id_type=MESH)
            for src, dst, s, r in ((code, code_in, code_send, code_recv), (scale, scale_in, scale_send, scale_recv))
        ]

    def received(way, t, d):
        for c in chunk_copies(way, t, d):
            c.wait_recv()
        return code_in[way, t, d].astype(jnp.int32).astype(jnp.float32) * scale_in[way, t, d][:1][None]

    def emit(t):
        def body(j, _):
            k = j // (2 * pieces)
            way = jnp.where(me < n // 2, j % 2, 1 - j % 2)
            d = jnp.where(way == 0, n - 1 - k, k)
            q = d * pieces + (j // 2) % pieces

            @pl.when(jnp.where(way == 0, d - me, me - d) > 0)
            def _():
                partial_sum(t, q, part)

                @pl.when(jnp.where(way == 0, me, n - 1 - me) > 0)
                def _():
                    part[...] += received(way, t, q)

                x = part[...]
                top = jnp.maximum(jnp.max(jnp.max(jnp.abs(x), axis=0), axis=0, keepdims=True), 1e-33)
                code[t, q] = jnp.round(x * (LEVELS / top)[None]).astype(jnp.int32).astype(jnp.int16)
                scale[t, q] = jnp.broadcast_to(top * (1.0 / LEVELS), (8, vectors))
                for c in chunk_copies(way, t, q):
                    c.start()
            return 0

        lax.fori_loop(0, 2 * pieces * (n - 1), body, 0)

    def forward(t):
        for o in range(1, n):
            eig_copy(t - 1, o, me).wait_send()
        for o in far_first[::-1]:
            eig_copy(t, o, me).start()

    for t in range(slices):
        if t + 1 < slices:
            @pl.when(is_end)
            def _():
                forward(t + 1)
        else:
            for o in range(1, n):
                eig_copy(t, o, me).wait_send()
        for o in range(1, n):
            source = lax.rem(me + n - o, n)
            if t == 0:
                eig_copy(t, o, source).wait_recv()
            else:
                @pl.when(is_end | (source != outer))
                def _():
                    eig_copy(t, o, source).wait_recv()
        if t + 1 < slices:
            @pl.when(jnp.logical_not(is_end))
            def _():
                o = lax.rem(me + n - outer, n)
                eig_copy(t + 1, o, outer).wait_recv()
                forward(t + 1)
        eig_own(t).wait()
        for c in range(2):
            w_v[t, c * vectors:(c + 1) * vectors, :] = (
                eig_v[t, :, c].astype(jnp.float32).reshape(vectors, cols).astype(jnp.bfloat16))

        def wait_sol(d, _):
            sol_copy(t, d).wait()
            return 0

        lax.fori_loop(0, n, wait_sol, 0)
        emit(t)

        def own_sum(i, _):
            partial_sum(t, me * pieces + i, own.at[t, i])
            return 0

        lax.fori_loop(0, pieces, own_sum, 0)

    def finish(j, _):
        t, i = j // pieces, j % pieces

        @pl.when(me > 0)
        def _():
            own[t, i] += received(0, t, me * pieces + i)

        @pl.when(me < n - 1)
        def _():
            own[t, i] += received(1, t, me * pieces + i)

        now = lax.axis_index("tm") * slices + t
        for b in range(piece):
            sign = jnp.where(now < time_ref[me * owned + i * piece + b], -1.0, 1.0)
            out_ref[t, i * piece + b] = (own[t, i, b] * sign).astype(jnp.bfloat16)
        return 0

    lax.fori_loop(0, slices * pieces, finish, 0)

    def drain(j, _):
        t, q = j // (n * pieces), j % (n * pieces)
        d = q // pieces

        @pl.when(d != me)
        def _():
            for c in chunk_copies(jnp.where(d > me, 0, 1), t, q):
                c.wait_send()
        return 0

    lax.fori_loop(0, slices * n * pieces, drain, 0)


def shards(n, solutions, eigvecs, source_time):
    slices, sources, spins, cols = solutions.shape
    count = eigvecs.shape[2]
    vectors = n * count
    owned = sources // n
    pieces = PIECES if owned % PIECES == 0 else 1
    piece = owned // pieces
    blocks = n * pieces
    dma = pltpu.SemaphoreType.DMA
    return pl.pallas_call(
        functools.partial(kernel, n, pieces),
        out_shape=jax.ShapeDtypeStruct((slices, owned, spins, vectors), jnp.bfloat16),
        in_specs=[
            pl.BlockSpec(memory_space=pltpu.HBM),
            pl.BlockSpec(memory_space=pltpu.HBM),
            pl.BlockSpec(memory_space=pltpu.HBM),
        ],
        out_specs=pl.BlockSpec(memory_space=pltpu.VMEM),
        scratch_shapes=[
            pltpu.SMEM(source_time.shape, jnp.int32),
            pltpu.VMEM(eigvecs.shape, jnp.bfloat16),
            pltpu.VMEM((slices, sources, spins, cols), jnp.bfloat16),
            pltpu.VMEM((slices, n, 2, count, cols), jnp.bfloat16),
            pltpu.VMEM((slices, 2 * vectors, cols), jnp.bfloat16),
            pltpu.VMEM((piece, spins, vectors), jnp.float32),
            pltpu.VMEM((slices, pieces, piece, spins, vectors), jnp.float32),
            pltpu.VMEM((slices, blocks, piece, spins, vectors), jnp.int16),
            pltpu.VMEM((slices, blocks, 8, vectors), jnp.float32),
            pltpu.VMEM((2, slices, blocks, piece, spins, vectors), jnp.int16),
            pltpu.VMEM((2, slices, blocks, 8, vectors), jnp.float32),
            dma,
            dma((slices,)),
            dma((slices, n)),
            dma((slices,)),
            dma((slices, n)),
            dma((slices, n)),
            dma((slices, blocks)),
            dma((slices, blocks)),
            dma((2, slices, blocks)),
            dma((2, slices, blocks)),
        ],
        compiler_params=pltpu.CompilerParams(
            collective_id=0, has_side_effects=True, vmem_limit_bytes=48 << 20),
    )(source_time, solutions, eigvecs)


def solution(mesh):
    return jax.shard_map(
        functools.partial(shards, mesh.shape["space"]),
        mesh=mesh,
        in_specs=(
            P(("cfg", "tm"), None, None, "space"),
            P(("cfg", "tm"), None, "space", None),
            P("cfg"),
        ),
        out_specs=P(("cfg", "tm"), "space", None, None),
        check_vma=False,
    )
```

```python
import functools

import jax
import jax.numpy as jnp
from jax import lax
from jax.experimental import pallas as pl
from jax.experimental.pallas import tpu as pltpu
from jax.sharding import PartitionSpec as P

MESH = pl.DeviceIdType.MESH
LEVELS = 32767.0
PIECES = 1
STEP = 0.6931471805599453 / 16


def kernel(n, pieces, time_hbm, sol_ref, eig_hbm, out_ref, time_ref, eig_ref, sol_v, eig_v, w_v, part, own, code,
           code_in, time_sem, load_sem, sol_sem, own_sem, eig_send, eig_recv, code_send, code_recv):
    me = lax.axis_index("space")
    slices, sources, spins, cols = sol_v.shape
    count = eig_ref.shape[2]
    vectors = n * count
    owned = sources // n
    piece = owned // pieces
    rows = piece * spins
    half = spins // 2
    outer = jnp.where(me < n // 2, me - 1, me + 1)
    is_end = (me == 0) | (me == n - 1)

    barrier = pltpu.get_barrier_semaphore()
    for o in range(1, n):
        pl.semaphore_signal(barrier, inc=1, device_id={"space": lax.rem(me + o, n)}, device_id_type=MESH)

    def block_of(d):
        return pl.ds(pl.multiple_of(d * cols, cols), cols)

    def eig_own(t):
        return pltpu.make_async_copy(eig_hbm.at[t, :, :, block_of(me)], eig_v.at[t, me], own_sem.at[t])

    def eig_load(t):
        return pltpu.make_async_copy(eig_hbm.at[t], eig_ref.at[t], load_sem.at[t])

    def sol_copy(t, d):
        rows = pl.ds(d * owned, owned)
        return pltpu.make_async_copy(sol_ref.at[t, rows], sol_v.at[t, rows], sol_sem.at[t, d])

    def eig_copy(t, o, dst):
        to = lax.rem(me + o, n)
        return pltpu.make_async_remote_copy(
            eig_ref.at[t, :, :, block_of(to)], eig_v.at[t, dst], eig_send.at[t, o], eig_recv.at[t, o],
            device_id={"space": to}, device_id_type=MESH)

    for t in range(slices):
        eig_load(t).start()
    time_copy = pltpu.make_async_copy(time_hbm, time_ref, time_sem)
    time_copy.start()
    for t in range(slices):
        eig_own(t).start()

    def start_sol(t):
        def body(d, _):
            sol_copy(t, d).start()
            return 0
        lax.fori_loop(0, n, body, 0)

    far_first = sorted(range(1, n), key=lambda o: -min(o, n - o))
    eig_load(0).wait()
    pl.semaphore_wait(barrier, n - 1)
    for o in far_first:
        eig_copy(0, o, me).start()
    for t in range(slices):
        start_sol(t)
    for t in range(1, slices):
        eig_load(t).wait()
    time_copy.wait()

    def partial_sum(t, q, dst):
        block = sol_v[t, pl.ds(q * piece, piece)].reshape(piece * spins, cols)
        p = lax.dot_general(block, w_v[t], (((1,), (1,)), ((), ())), preferred_element_type=jnp.float32)
        p = p.reshape(piece, 2, half, 2 * vectors)
        dst[:, :half, :] = p[:, 0, :, :vectors] + p[:, 1, :, vectors:]
        dst[:, half:, :] = p[:, 1, :, :vectors] - p[:, 0, :, vectors:]

    def chunk_copy(way, t, q):
        to = lax.rem(jnp.where(way == 0, me + 1, me + n - 1), n)
        return pltpu.make_async_remote_copy(
            code.at[t, q], code_in.at[way, t, q], code_send.at[t, q], code_recv.at[way, t, q],
            device_id={"space": to}, device_id_type=MESH)

    def received(way, t, q):
        chunk_copy(way, t, q).wait_recv()
        steps = code_in[way, t, q, rows:].astype(jnp.int32).astype(jnp.float32)[:1]
        value = code_in[way, t, q, :rows].astype(jnp.int32).astype(jnp.float32) * (jnp.exp(steps * STEP) * (1.0 / LEVELS))
        return value.reshape(piece, spins, vectors)

    def emit(t, way, d, i):
        q = d * pieces + i
        partial_sum(t, q, part)

        @pl.when(jnp.where(way == 0, me, n - 1 - me) > 0)
        def _():
            part[...] += received(way, t, q)

        x = part[...].reshape(rows, vectors)
        top = jnp.maximum(jnp.max(jnp.abs(x), axis=0, keepdims=True), 1e-30)
        steps = jnp.floor(jnp.log(top) * (1.0 / STEP)) + 2.0
        code[t, q, :rows] = jnp.round(x * (LEVELS * jnp.exp(steps * -STEP))).astype(jnp.int32).astype(jnp.int16)
        code[t, q, rows:] = jnp.broadcast_to(steps, (16, vectors)).astype(jnp.int32).astype(jnp.int16)
        chunk_copy(way, t, q).start()

    def emit_first(t):
        def body(j, _):
            k = j // (2 * pieces)
            way = jnp.where(me < n // 2, j % 2, 1 - j % 2)
            d = jnp.where(way == 0, n - 1 - k, k)
            least = jnp.where(is_end, 1, 0)

            @pl.when(jnp.where(way == 0, d - me, me - d) > least)
            def _():
                emit(t, way, d, (j // 2) % pieces)
            return 0

        lax.fori_loop(0, 2 * pieces * (n - 1), body, 0)

    def emit_last():
        def body(j, _):
            way = jnp.where(me == 0, 0, 1)
            emit(j // pieces, way, jnp.where(me == 0, 1, n - 2), j % pieces)
            return 0

        @pl.when(is_end)
        def _():
            lax.fori_loop(0, slices * pieces, body, 0)

    def forward(t):
        for o in range(1, n):
            eig_copy(t - 1, o, me).wait_send()
        for o in far_first[::-1]:
            eig_copy(t, o, me).start()

    for t in range(slices):
        if t + 1 < slices:
            @pl.when(is_end)
            def _():
                forward(t + 1)
        else:
            for o in range(1, n):
                eig_copy(t, o, me).wait_send()
        for o in range(1, n):
            source = lax.rem(me + n - o, n)
            if t == 0:
                eig_copy(t, o, source).wait_recv()
            else:
                @pl.when(is_end | (source != outer))
                def _():
                    eig_copy(t, o, source).wait_recv()
        if t + 1 < slices:
            @pl.when(jnp.logical_not(is_end))
            def _():
                o = lax.rem(me + n - outer, n)
                eig_copy(t + 1, o, outer).wait_recv()
                forward(t + 1)
        eig_own(t).wait()
        for c in range(2):
            w_v[t, c * vectors:(c + 1) * vectors, :] = (
                eig_v[t, :, c].astype(jnp.float32).reshape(vectors, cols).astype(jnp.bfloat16))

        def wait_sol(d, _):
            sol_copy(t, d).wait()
            return 0

        lax.fori_loop(0, n, wait_sol, 0)
        emit_first(t)
        if t + 1 == slices:
            emit_last()

        def own_sum(i, _):
            partial_sum(t, me * pieces + i, own.at[t, i])
            return 0

        lax.fori_loop(0, pieces, own_sum, 0)

    def finish(j, _):
        t, i = j // pieces, j % pieces

        @pl.when(me > 0)
        def _():
            own[t, i] += received(0, t, me * pieces + i)

        @pl.when(me < n - 1)
        def _():
            own[t, i] += received(1, t, me * pieces + i)

        now = lax.axis_index("tm") * slices + t
        for b in range(piece):
            sign = jnp.where(now < time_ref[me * owned + i * piece + b], -1.0, 1.0)
            out_ref[t, i * piece + b] = (own[t, i, b] * sign).astype(jnp.bfloat16)
        return 0

    lax.fori_loop(0, slices * pieces, finish, 0)

    def drain(j, _):
        t, q = j // (n * pieces), j % (n * pieces)
        d = q // pieces

        @pl.when(d != me)
        def _():
            chunk_copy(jnp.where(d > me, 0, 1), t, q).wait_send()
        return 0

    lax.fori_loop(0, slices * n * pieces, drain, 0)


def shards(n, solutions, eigvecs, source_time):
    slices, sources, spins, cols = solutions.shape
    count = eigvecs.shape[2]
    vectors = n * count
    owned = sources // n
    pieces = PIECES if owned % PIECES == 0 else 1
    piece = owned // pieces
    blocks = n * pieces
    dma = pltpu.SemaphoreType.DMA
    return pl.pallas_call(
        functools.partial(kernel, n, pieces),
        out_shape=jax.ShapeDtypeStruct((slices, owned, spins, vectors), jnp.bfloat16),
        in_specs=[
            pl.BlockSpec(memory_space=pltpu.HBM),
            pl.BlockSpec(memory_space=pltpu.HBM),
            pl.BlockSpec(memory_space=pltpu.HBM),
        ],
        out_specs=pl.BlockSpec(memory_space=pltpu.VMEM),
        scratch_shapes=[
            pltpu.SMEM(source_time.shape, jnp.int32),
            pltpu.VMEM(eigvecs.shape, jnp.bfloat16),
            pltpu.VMEM((slices, sources, spins, cols), jnp.bfloat16),
            pltpu.VMEM((slices, n, 2, count, cols), jnp.bfloat16),
            pltpu.VMEM((slices, 2 * vectors, cols), jnp.bfloat16),
            pltpu.VMEM((piece, spins, vectors), jnp.float32),
            pltpu.VMEM((slices, pieces, piece, spins, vectors), jnp.float32),
            pltpu.VMEM((slices, blocks, piece * spins + 16, vectors), jnp.int16),
            pltpu.VMEM((2, slices, blocks, piece * spins + 16, vectors), jnp.int16),
            dma,
            dma((slices,)),
            dma((slices, n)),
            dma((slices,)),
            dma((slices, n)),
            dma((slices, n)),
            dma((slices, blocks)),
            dma((2, slices, blocks)),
        ],
        compiler_params=pltpu.CompilerParams(
            collective_id=0, has_side_effects=True, vmem_limit_bytes=48 << 20),
    )(source_time, solutions, eigvecs)


def solution(mesh):
    return jax.shard_map(
        functools.partial(shards, mesh.shape["space"]),
        mesh=mesh,
        in_specs=(
            P(("cfg", "tm"), None, None, "space"),
            P(("cfg", "tm"), None, "space", None),
            P("cfg"),
        ),
        out_specs=P(("cfg", "tm"), "space", None, None),
        check_vma=False,
    )
```

```python
import functools

import jax
import jax.numpy as jnp
from jax import lax
from jax.experimental import pallas as pl
from jax.experimental.pallas import tpu as pltpu
from jax.sharding import PartitionSpec as P

MESH = pl.DeviceIdType.MESH
LEVELS = 32767.0
PIECES = 1
STEP = 0.6931471805599453 / 16


def kernel(n, pieces, time_hbm, sol_ref, eig_hbm, out_ref, time_ref, eig_ref, sol_v, eig_v, w_v, part, own, code,
           code_in, time_sem, load_sem, sol_sem, own_sem, eig_send, eig_recv, code_send, code_recv, wave):
    me = lax.axis_index("space")
    slices, sources, spins, cols = sol_v.shape
    count = eig_ref.shape[2]
    vectors = n * count
    owned = sources // n
    piece = owned // pieces
    rows = piece * spins
    half = spins // 2
    outer = jnp.where(me < n // 2, me - 1, me + 1)
    is_end = (me == 0) | (me == n - 1)

    barrier = pltpu.get_barrier_semaphore()

    def tell(semaphore, where):
        pl.semaphore_signal(semaphore, inc=1, device_id={"space": lax.rem(where + n, n)}, device_id_type=MESH)

    @pl.when(me > 0)
    def _():
        tell(barrier, me - 1)

    @pl.when(me < n - 1)
    def _():
        tell(barrier, me + 1)

    def block_of(d):
        return pl.ds(pl.multiple_of(d * cols, cols), cols)

    def eig_own(t):
        return pltpu.make_async_copy(eig_hbm.at[t, :, :, block_of(me)], eig_v.at[t, me], own_sem.at[t])

    def eig_load(t):
        return pltpu.make_async_copy(eig_hbm.at[t], eig_ref.at[t], load_sem.at[t])

    def sol_copy(t, d):
        rows = pl.ds(d * owned, owned)
        return pltpu.make_async_copy(sol_ref.at[t, rows], sol_v.at[t, rows], sol_sem.at[t, d])

    def eig_copy(t, o, dst):
        to = lax.rem(me + o, n)
        return pltpu.make_async_remote_copy(
            eig_ref.at[t, :, :, block_of(to)], eig_v.at[t, dst], eig_send.at[t, o], eig_recv.at[t, o],
            device_id={"space": to}, device_id_type=MESH)

    for t in range(slices):
        eig_load(t).start()
    time_copy = pltpu.make_async_copy(time_hbm, time_ref, time_sem)
    time_copy.start()
    for t in range(slices):
        eig_own(t).start()

    def start_sol(t):
        def body(d, _):
            sol_copy(t, d).start()
            return 0
        lax.fori_loop(0, n, body, 0)

    far_first = sorted(range(1, n), key=lambda o: -min(o, n - o))
    eig_load(0).wait()
    pl.semaphore_wait(barrier, jnp.where(is_end, 1, 2))

    def is_near(o):
        return jnp.abs(lax.rem(me + o, n) - me) == 1

    @pl.when(me == 0)
    def _():
        tell(wave.at[0], me + 1)

    @pl.when(me == n - 1)
    def _():
        tell(wave.at[1], me - 1)

    for o in far_first:
        @pl.when(is_near(o))
        def _():
            eig_copy(0, o, me).start()

    @pl.when(me > 0)
    def _():
        pl.semaphore_wait(wave.at[0], 1)

        @pl.when(me < n - 1)
        def _():
            tell(wave.at[0], me + 1)

    @pl.when(me < n - 1)
    def _():
        pl.semaphore_wait(wave.at[1], 1)

        @pl.when(me > 0)
        def _():
            tell(wave.at[1], me - 1)

    for o in far_first:
        @pl.when(jnp.logical_not(is_near(o)))
        def _():
            eig_copy(0, o, me).start()
    for t in range(slices):
        start_sol(t)
    for t in range(1, slices):
        eig_load(t).wait()
    time_copy.wait()

    def partial_sum(t, q, dst):
        block = sol_v[t, pl.ds(q * piece, piece)].reshape(piece * spins, cols)
        p = lax.dot_general(block, w_v[t], (((1,), (1,)), ((), ())), preferred_element_type=jnp.float32)
        p = p.reshape(piece, 2, half, 2 * vectors)
        dst[:, :half, :] = p[:, 0, :, :vectors] + p[:, 1, :, vectors:]
        dst[:, half:, :] = p[:, 1, :, :vectors] - p[:, 0, :, vectors:]

    def chunk_copy(way, t, q):
        to = lax.rem(jnp.where(way == 0, me + 1, me + n - 1), n)
        return pltpu.make_async_remote_copy(
            code.at[t, q], code_in.at[way, t, q], code_send.at[t, q], code_recv.at[way, t, q],
            device_id={"space": to}, device_id_type=MESH)

    def received(way, t, q):
        chunk_copy(way, t, q).wait_recv()
        steps = code_in[way, t, q, rows:].astype(jnp.int32).astype(jnp.float32)[:1]
        value = code_in[way, t, q, :rows].astype(jnp.int32).astype(jnp.float32) * (jnp.exp(steps * STEP) * (1.0 / LEVELS))
        return value.reshape(piece, spins, vectors)

    def emit(t, way, d, i):
        q = d * pieces + i
        partial_sum(t, q, part)

        @pl.when(jnp.where(way == 0, me, n - 1 - me) > 0)
        def _():
            part[...] += received(way, t, q)

        x = part[...].reshape(rows, vectors)
        top = jnp.maximum(jnp.max(jnp.abs(x), axis=0, keepdims=True), 1e-30)
        steps = jnp.floor(jnp.log(top) * (1.0 / STEP)) + 2.0
        code[t, q, :rows] = jnp.round(x * (LEVELS * jnp.exp(steps * -STEP))).astype(jnp.int32).astype(jnp.int16)
        code[t, q, rows:] = jnp.broadcast_to(steps, (16, vectors)).astype(jnp.int32).astype(jnp.int16)
        chunk_copy(way, t, q).start()

    def emit_first(t):
        def body(j, _):
            k = j // (2 * pieces)
            way = jnp.where(me < n // 2, j % 2, 1 - j % 2)
            d = jnp.where(way == 0, n - 1 - k, k)
            least = jnp.where(is_end, 1, 0)

            @pl.when(jnp.where(way == 0, d - me, me - d) > least)
            def _():
                emit(t, way, d, (j // 2) % pieces)
            return 0

        lax.fori_loop(0, 2 * pieces * (n - 1), body, 0)

    def emit_last():
        def body(j, _):
            way = jnp.where(me == 0, 0, 1)
            emit(j // pieces, way, jnp.where(me == 0, 1, n - 2), j % pieces)
            return 0

        @pl.when(is_end)
        def _():
            lax.fori_loop(0, slices * pieces, body, 0)

    def forward(t):
        for o in range(1, n):
            eig_copy(t - 1, o, me).wait_send()
        for o in far_first[::-1]:
            eig_copy(t, o, me).start()

    for t in range(slices):
        if t + 1 < slices:
            @pl.when(is_end)
            def _():
                forward(t + 1)
        else:
            for o in range(1, n):
                eig_copy(t, o, me).wait_send()
        for o in range(1, n):
            source = lax.rem(me + n - o, n)
            if t == 0:
                eig_copy(t, o, source).wait_recv()
            else:
                @pl.when(is_end | (source != outer))
                def _():
                    eig_copy(t, o, source).wait_recv()
        if t + 1 < slices:
            @pl.when(jnp.logical_not(is_end))
            def _():
                o = lax.rem(me + n - outer, n)
                eig_copy(t + 1, o, outer).wait_recv()
                forward(t + 1)
        eig_own(t).wait()
        for c in range(2):
            w_v[t, c * vectors:(c + 1) * vectors, :] = (
                eig_v[t, :, c].astype(jnp.float32).reshape(vectors, cols).astype(jnp.bfloat16))

        def wait_sol(d, _):
            sol_copy(t, d).wait()
            return 0

        lax.fori_loop(0, n, wait_sol, 0)
        emit_first(t)
        if t + 1 == slices:
            emit_last()

        def own_sum(i, _):
            partial_sum(t, me * pieces + i, own.at[t, i])
            return 0

        lax.fori_loop(0, pieces, own_sum, 0)

    def finish(j, _):
        t, i = j // pieces, j % pieces

        @pl.when(me > 0)
        def _():
            own[t, i] += received(0, t, me * pieces + i)

        @pl.when(me < n - 1)
        def _():
            own[t, i] += received(1, t, me * pieces + i)

        now = lax.axis_index("tm") * slices + t
        for b in range(piece):
            sign = jnp.where(now < time_ref[me * owned + i * piece + b], -1.0, 1.0)
            out_ref[t, i * piece + b] = (own[t, i, b] * sign).astype(jnp.bfloat16)
        return 0

    lax.fori_loop(0, slices * pieces, finish, 0)

    def drain(j, _):
        t, q = j // (n * pieces), j % (n * pieces)
        d = q // pieces

        @pl.when(d != me)
        def _():
            chunk_copy(jnp.where(d > me, 0, 1), t, q).wait_send()
        return 0

    lax.fori_loop(0, slices * n * pieces, drain, 0)


def shards(n, solutions, eigvecs, source_time):
    slices, sources, spins, cols = solutions.shape
    count = eigvecs.shape[2]
    vectors = n * count
    owned = sources // n
    pieces = PIECES if owned % PIECES == 0 else 1
    piece = owned // pieces
    blocks = n * pieces
    dma = pltpu.SemaphoreType.DMA
    return pl.pallas_call(
        functools.partial(kernel, n, pieces),
        out_shape=jax.ShapeDtypeStruct((slices, owned, spins, vectors), jnp.bfloat16),
        in_specs=[
            pl.BlockSpec(memory_space=pltpu.HBM),
            pl.BlockSpec(memory_space=pltpu.HBM),
            pl.BlockSpec(memory_space=pltpu.HBM),
        ],
        out_specs=pl.BlockSpec(memory_space=pltpu.VMEM),
        scratch_shapes=[
            pltpu.SMEM(source_time.shape, jnp.int32),
            pltpu.VMEM(eigvecs.shape, jnp.bfloat16),
            pltpu.VMEM((slices, sources, spins, cols), jnp.bfloat16),
            pltpu.VMEM((slices, n, 2, count, cols), jnp.bfloat16),
            pltpu.VMEM((slices, 2 * vectors, cols), jnp.bfloat16),
            pltpu.VMEM((piece, spins, vectors), jnp.float32),
            pltpu.VMEM((slices, pieces, piece, spins, vectors), jnp.float32),
            pltpu.VMEM((slices, blocks, piece * spins + 16, vectors), jnp.int16),
            pltpu.VMEM((2, slices, blocks, piece * spins + 16, vectors), jnp.int16),
            dma,
            dma((slices,)),
            dma((slices, n)),
            dma((slices,)),
            dma((slices, n)),
            dma((slices, n)),
            dma((slices, blocks)),
            dma((2, slices, blocks)),
            pltpu.SemaphoreType.REGULAR((2,)),
        ],
        compiler_params=pltpu.CompilerParams(
            collective_id=0, has_side_effects=True, vmem_limit_bytes=48 << 20),
    )(source_time, solutions, eigvecs)


def solution(mesh):
    return jax.shard_map(
        functools.partial(shards, mesh.shape["space"]),
        mesh=mesh,
        in_specs=(
            P(("cfg", "tm"), None, None, "space"),
            P(("cfg", "tm"), None, "space", None),
            P("cfg"),
        ),
        out_specs=P(("cfg", "tm"), "space", None, None),
        check_vma=False,
    )
```
